32 devices in a mesh: band: 8 (over z, x), sub: 4 (over y, core).
Axes of the slice: x: 2, y: 2, z: 4, core: 2. Of those that a mesh axis runs over, the one named last changes fastest.
Arguments:
- grad_pred: bfloat16 [227, 24576], P(None, ('band', 'sub')), may hold values from -6 to 6
- grid_latent: bfloat16 [24576, 512], P(('band', 'sub')), may hold values from -6 to 6
- mesh_latent: bfloat16 [10240, 512], P(('band', 'sub')), may hold values from -6 to 6
- send_slot: int32 [24576], P(('band', 'sub')), may hold values from 0 to 2303, as said below
- edge_src: int32 [3, 73728], P(None, ('band', 'sub')), may hold values from 0 to 10239, as said below
- w_mesh: bfloat16 [512, 512], replicated, may hold values from -0.25 to 0.25
- w_grid: bfloat16 [512, 512], replicated, may hold values from -0.25 to 0.25
- w_msg: bfloat16 [512, 512], replicated, may hold values from -0.25 to 0.25
- w_out: bfloat16 [512, 227], replicated, may hold values from -0.25 to 0.25
Outputs:
- mesh_grad: bfloat16 [10240, 512], P(('band', 'sub'))
- grad_w_mesh: float32 [512, 512], replicated
- grad_w_grid: float32 [512, 512], replicated
- grad_w_msg: float32 [512, 512], replicated
- grad_w_out: float32 [512, 227], replicated
The draws below stay inside these ranges and needn't reach their ends.
Inputs may be any that keep to these rules, and one draw needn't show every extreme that they name: For grid point p on latitude-major device i, send_slot[p] = j * 72 + r names patch-major device j and a rank r. On one device i the values are distinct, and for each j the ranks used are 0 to the count of i's points sent to j minus 1. Every such count is at most 72, and 72 is reached in every draw. Every grid point thereby gets one patch-major slot; live slots of each source stand at the front of its block of 72. One patch-major device holds at most 1920 live slots, reached on some device in every draw. `edge_src`: A slot on patch-major device j, of band b = j // 4, names senders in patch b only: mesh rows b * 1280 to (b + 1) * 1280 - 1. Entries of empty slots lie in that range too and are not read.
All inputs are finite; a program needn't handle non-finite values.
Results may differ from the reference program's by a relative error of at most 0.0076.
Values may be sent and summed in bfloat16 or wider, within the bound.
A program may use at most 128 MiB of HBM per device.

```python
import math
import jax
import jax.numpy as jnp

D = 512
C = 227
G_DEV = 768
GRID = 24576
MESH = 10240
PATCH = 1280
CAP = 72
SLOT_DEV = 2304
SLOTS = 73728
N_BAND = 8
N_SUB = 4
DEVICES = 32


def relay_table(key):
    base_count = G_DEV // DEVICES
    half_base = base_count // 2
    receivers = jnp.arange(DEVICES, dtype=jnp.int32)
    band_index = receivers // N_SUB
    polar_band = (band_index < N_BAND // 8) | (band_index >= N_BAND - N_BAND // 8)
    receive_load = jnp.where(polar_band, 5 * half_base, half_base).astype(jnp.int32)
    draw_key, shuffle_key = jax.random.split(jax.random.fold_in(key, 7))
    increments = jax.random.randint(draw_key, (DEVICES,), 0, half_base + 1)
    increments = increments.at[0].set(half_base).at[DEVICES - 1].set(0)
    offsets = (increments - jnp.roll(increments, 1)).astype(jnp.int32)
    senders = jnp.arange(DEVICES, dtype=jnp.int32)
    counts = receive_load[None, :] + offsets[(receivers[None, :] - senders[:, None]) % DEVICES]
    block_ends = jnp.cumsum(counts, axis=1)
    starts = block_ends - counts
    positions = jnp.arange(G_DEV, dtype=jnp.int32)

    def one_sender(row_ends, row_starts, sub_key):
        target = jnp.sum((row_ends[None, :] <= positions[:, None]).astype(jnp.int32), axis=1)
        slot_rank = positions - row_starts[target]
        shuffle = jax.random.permutation(sub_key, G_DEV)
        return jnp.zeros((G_DEV,), jnp.int32).at[shuffle].set(target * CAP + slot_rank)
    sender_keys = jax.random.split(shuffle_key, DEVICES)
    table = jax.vmap(one_sender)(block_ends, starts, sender_keys)
    return table.reshape(GRID).astype(jnp.int32)


def draw_send_slot(key, part):
    return relay_table(key)


def draw_edge_src(key, part):
    local_node = jax.random.randint(jax.random.fold_in(key, 11), (3, SLOTS), 0, PATCH)
    holders = jnp.arange(SLOTS, dtype=jnp.int32) // SLOT_DEV
    band_index = holders // N_SUB
    return (local_node + band_index[None, :] * PATCH).astype(jnp.int32)


def steps_of(rng, shape, cuts, low, largest):
    def one(dim, blocks):
        steps = jax.random.uniform(jax.random.fold_in(jax.random.fold_in(rng, 6), dim), (blocks,), jnp.float32, low / len(cuts), largest / len(cuts))
        return jnp.repeat(jnp.exp(steps), shape[dim] // blocks).reshape((-1,) + (1,) * (len(shape) - dim - 1))

    loudness = one(*cuts[0])
    for cut in cuts[1:]:
        loudness = loudness * one(*cut)
    return loudness


def bell_draw(rng, dims, scale, bound, cuts=(), kind=jnp.bfloat16):
    factor_of = steps_of(rng, dims, cuts, -0.22, 0.18) if cuts else 1.0
    values = jax.random.normal(rng, dims, jnp.float32) * scale * factor_of
    return jnp.minimum(jnp.maximum(values, -bound), bound).astype(kind)


def setup_inputs(seed: int = 0) -> dict:
    seeds = jax.random.split(jax.random.key(seed), 10)
    grad_pred = bell_draw(seeds[0], (C, GRID), 1.0, 6.0, ((1, 32),))
    grid_latent = bell_draw(seeds[1], (GRID, D), 1.0, 6.0, ((0, 32),))
    mesh_latent = bell_draw(seeds[2], (MESH, D), 1.0, 6.0, ((0, 32),))
    send_slot = draw_send_slot(jax.random.fold_in(seeds[9], 71), 0)
    edge_src = draw_edge_src(jax.random.fold_in(seeds[9], 71), 0)
    w_mesh = bell_draw(seeds[5], (D, D), D ** -0.5, 0.25)
    w_grid = bell_draw(seeds[6], (D, D), D ** -0.5, 0.25)
    w_msg = bell_draw(seeds[7], (D, D), D ** -0.5, 0.25)
    w_out = bell_draw(seeds[8], (D, C), D ** -0.5, 0.25)
    return {"grad_pred": grad_pred, "grid_latent": grid_latent, "mesh_latent": mesh_latent, "send_slot": send_slot, "edge_src": edge_src, "w_mesh": w_mesh, "w_grid": w_grid, "w_msg": w_msg, "w_out": w_out}


def latitude_weight(points, total):
    angle = jnp.pi * ((points.astype(jnp.float32) + 0.5) / total - 0.5)
    return 0.5 * jnp.pi * jnp.cos(angle)

def silu_slope(value):
    sigma = jax.nn.sigmoid(value)
    return sigma * (1.0 + value * (1.0 - sigma))

def reference(grad_pred, grid_latent, mesh_latent, send_slot, edge_src, w_mesh, w_grid, w_msg, w_out):
    points = jnp.arange(GRID, dtype=jnp.int32)
    source_dev = (points // G_DEV).astype(jnp.int32)
    target = (send_slot // CAP).astype(jnp.int32)
    slot_rank = (send_slot % CAP).astype(jnp.int32)
    holder = (target * SLOT_DEV + source_dev * CAP + slot_rank).astype(jnp.int32)
    senders = edge_src[:, holder]
    grid_proj = jnp.dot(grid_latent, w_grid, preferred_element_type=jnp.float32).astype(jnp.bfloat16)
    mesh_proj = jnp.dot(mesh_latent, w_mesh, preferred_element_type=jnp.float32).astype(jnp.bfloat16)
    grid_float = grid_proj.astype(jnp.float32)
    pre_acts = [mesh_proj[senders[corner]].astype(jnp.float32) + grid_float for corner in range(3)]
    act_sum = (jax.nn.silu(pre_acts[0]) + jax.nn.silu(pre_acts[1]) + jax.nn.silu(pre_acts[2])).astype(jnp.bfloat16)
    aggregate = jnp.dot(act_sum, w_msg, preferred_element_type=jnp.float32).astype(jnp.bfloat16)
    weighted = (latitude_weight(points, GRID)[None, :] * grad_pred.astype(jnp.float32)).astype(jnp.bfloat16)
    raw_out = jnp.dot(aggregate.T, weighted.T, preferred_element_type=jnp.float32)
    agg_grad = jnp.dot(weighted.T, w_out.T, preferred_element_type=jnp.float32).astype(jnp.bfloat16)
    raw_msg = jnp.dot(act_sum.T, agg_grad, preferred_element_type=jnp.float32)
    act_grad = jnp.dot(agg_grad, w_msg.T, preferred_element_type=jnp.float32)
    pre_grads = [(act_grad * silu_slope(pre)).astype(jnp.bfloat16) for pre in pre_acts]
    grid_proj_grad = (pre_grads[0].astype(jnp.float32) + pre_grads[1].astype(jnp.float32) + pre_grads[2].astype(jnp.float32)).astype(jnp.bfloat16)
    raw_grid = jnp.dot(grid_latent.T, grid_proj_grad, preferred_element_type=jnp.float32)
    node_total = jnp.zeros((MESH, D), jnp.float32)
    for corner in range(3):
        node_total = node_total.at[senders[corner]].add(pre_grads[corner].astype(jnp.float32))
    mesh_proj_grad = node_total.astype(jnp.bfloat16)
    mesh_grad = jnp.dot(mesh_proj_grad, w_mesh.T, preferred_element_type=jnp.float32).astype(jnp.bfloat16)
    raw_mesh = jnp.dot(mesh_latent.T, mesh_proj_grad, preferred_element_type=jnp.float32)
    grad_scale = 1.0 / math.sqrt(3.0 * GRID)
    return (mesh_grad, raw_mesh * grad_scale, raw_grid * grad_scale, raw_msg * grad_scale, raw_out * grad_scale)
```

```python
import math

import jax
import jax.numpy as jnp
from jax import lax
from jax.sharding import PartitionSpec as P


def latitude_weight(points, total):
    angle = jnp.pi * ((points.astype(jnp.float32) + 0.5) / total - 0.5)
    return 0.5 * jnp.pi * jnp.cos(angle)


def silu_slope(value):
    sigma = jax.nn.sigmoid(value)
    return sigma * (1.0 + value * (1.0 - sigma))


def contract_rows(left, right):
    return lax.dot_general(
        left, right, (((0,), (0,)), ((), ())), preferred_element_type=jnp.float32
    )


def times_transpose(left, right):
    return lax.dot_general(
        left, right, (((1,), (1,)), ((), ())), preferred_element_type=jnp.float32
    )


def spread(rows, index, slots):
    places = lax.broadcasted_iota(jnp.int32, (slots, index.shape[0]), 0)
    return (places == index[None, :]).astype(rows.dtype)


def shards(grad_pred, grid_latent, mesh_latent, send_slot, edge_src, w_mesh, w_grid, w_msg, w_out):
    both = ("band", "sub")
    grid_rows, width = grid_latent.shape
    channels = grad_pred.shape[0]
    devices = lax.axis_size(both)
    subs = lax.axis_size("sub")
    capacity = 3 * grid_rows // devices
    total_points = grid_rows * devices
    slots = devices * capacity
    own_index = lax.axis_index(both)
    points = own_index * grid_rows + jnp.arange(grid_rows, dtype=jnp.int32)
    weighted = (
        latitude_weight(points, total_points)[None, :] * grad_pred.astype(jnp.float32)
    ).astype(jnp.bfloat16)
    one_hot = spread(grid_latent, send_slot, slots)
    latent_send = jnp.dot(one_hot, grid_latent, preferred_element_type=jnp.float32).astype(
        jnp.bfloat16
    )
    grad_send = times_transpose(one_hot, weighted).astype(jnp.bfloat16)
    latent_rows = lax.all_to_all(
        latent_send.reshape(devices, capacity, width), both, split_axis=0, concat_axis=0, tiled=True
    ).reshape(slots, width)
    grad_rows = lax.all_to_all(
        grad_send.reshape(devices, capacity, channels), both, split_axis=0, concat_axis=0, tiled=True
    ).reshape(slots, channels)
    patch_latent = lax.all_gather(mesh_latent, "sub", axis=0, tiled=True)
    patch_size = patch_latent.shape[0]
    patch_proj = jnp.dot(patch_latent, w_mesh, preferred_element_type=jnp.float32).astype(
        jnp.bfloat16
    )
    local_node = edge_src - lax.axis_index("band") * patch_size
    nodes = lax.broadcasted_iota(jnp.int32, (slots, patch_size), 1)
    grid_float = (
        jnp.dot(latent_rows, w_grid, preferred_element_type=jnp.float32)
        .astype(jnp.bfloat16)
        .astype(jnp.float32)
    )
    pre_acts = [
        jnp.dot(
            (nodes == local_node[corner][:, None]).astype(jnp.bfloat16),
            patch_proj,
            preferred_element_type=jnp.float32,
        )
        + grid_float
        for corner in range(3)
    ]
    act_sum = (
        jax.nn.silu(pre_acts[0]) + jax.nn.silu(pre_acts[1]) + jax.nn.silu(pre_acts[2])
    ).astype(jnp.bfloat16)
    aggregate = jnp.dot(act_sum, w_msg, preferred_element_type=jnp.float32).astype(jnp.bfloat16)
    out_part = contract_rows(aggregate, grad_rows)
    agg_rows = times_transpose(grad_rows, w_out).astype(jnp.bfloat16)
    msg_part = contract_rows(act_sum, agg_rows)
    act_grad = times_transpose(agg_rows, w_msg)
    pre_grads = [(act_grad * silu_slope(pre)).astype(jnp.bfloat16) for pre in pre_acts]
    grid_proj_grad = (
        pre_grads[0].astype(jnp.float32)
        + pre_grads[1].astype(jnp.float32)
        + pre_grads[2].astype(jnp.float32)
    ).astype(jnp.bfloat16)
    targets = lax.broadcasted_iota(jnp.int32, (patch_size, slots), 0)
    node_part = sum(
        jnp.dot(
            (targets == local_node[corner][None, :]).astype(jnp.bfloat16),
            pre_grads[corner],
            preferred_element_type=jnp.float32,
        )
        for corner in range(3)
    ).astype(jnp.bfloat16)
    node_parts = lax.all_to_all(
        node_part.reshape(subs, patch_size // subs, width),
        "sub",
        split_axis=0,
        concat_axis=0,
        tiled=True,
    )
    grid_part = contract_rows(latent_rows, grid_proj_grad)
    mesh_part = contract_rows(patch_latent, node_part)
    parts = jnp.concatenate([mesh_part, grid_part, msg_part, out_part], axis=1).astype(jnp.bfloat16)
    exchanged = lax.all_to_all(
        parts.reshape(devices, width // devices, parts.shape[1]),
        both,
        split_axis=0,
        concat_axis=0,
        tiled=True,
    )
    own_rows = jnp.sum(exchanged.astype(jnp.float32), axis=0).astype(jnp.bfloat16)
    totals = lax.all_gather(own_rows, both, axis=0, tiled=True)
    mesh_proj_grad = jnp.sum(node_parts.astype(jnp.float32), axis=0).astype(jnp.bfloat16)
    mesh_grad = times_transpose(mesh_proj_grad, w_mesh).astype(jnp.bfloat16)
    grad_scale = 1.0 / math.sqrt(3.0 * total_points)
    scaled = totals.astype(jnp.float32) * grad_scale
    return (
        mesh_grad,
        scaled[:, :width],
        scaled[:, width : 2 * width],
        scaled[:, 2 * width : 3 * width],
        scaled[:, 3 * width :],
    )


def solution(mesh):
    placed = (
        P(None, ("band", "sub")),
        P(("band", "sub"), None),
        P(("band", "sub"), None),
        P(("band", "sub")),
        P(None, ("band", "sub")),
        P(),
        P(),
        P(),
        P(),
    )
    return jax.shard_map(
        shards,
        mesh=mesh,
        in_specs=placed,
        out_specs=(P(("band", "sub"), None), P(), P(), P(), P()),
        check_vma=False,
    )
```

```python
import functools
import math

import jax
import jax.numpy as jnp
from jax import lax
from jax.experimental import pallas as pl
from jax.experimental.pallas import tpu as pltpu
from jax.sharding import PartitionSpec as P


def latitude_weight(points, total):
    angle = jnp.pi * ((points.astype(jnp.float32) + 0.5) / total - 0.5)
    return 0.5 * jnp.pi * jnp.cos(angle)


def silu_slope(value):
    sigma = jax.nn.sigmoid(value)
    return sigma * (1.0 + value * (1.0 - sigma))


def contract_rows(left, right):
    return lax.dot_general(
        left, right, (((0,), (0,)), ((), ())), preferred_element_type=jnp.float32
    )


def times_transpose(left, right):
    return lax.dot_general(
        left, right, (((1,), (1,)), ((), ())), preferred_element_type=jnp.float32
    )


def spread(rows, index, slots):
    places = lax.broadcasted_iota(jnp.int32, (slots, index.shape[0]), 0)
    return (places == index[None, :]).astype(rows.dtype)


def reduce_kernel(
    subs,
    parts_ref,
    nodes_ref,
    total_ref,
    node_ref,
    half_in,
    half_sum,
    group_in,
    node_in,
    node_sum,
    node_last,
    half_sem,
    group_send,
    group_recv,
    own_send,
    own_recv,
    pass_send,
    pass_recv,
    node_send,
    node_recv,
    last_send,
    last_recv,
):
    devices = parts_ref.shape[0]
    groups = devices // 2
    sub_groups = subs // 2
    band, sub = lax.axis_index("band"), lax.axis_index("sub")
    me = band * subs + sub
    parity, group = me % 2, me // 2
    other = 1 - parity
    partner = me + 1 - 2 * parity
    own_pair = sub // 2

    def remote(src, dst, send_sem, recv_sem, device):
        return pltpu.make_async_remote_copy(
            src_ref=src,
            dst_ref=dst,
            send_sem=send_sem,
            recv_sem=recv_sem,
            device_id=(device // subs, device % subs),
            device_id_type=pl.DeviceIdType.MESH,
        )

    def member(index):
        return 2 * index + parity

    def ahead(step):
        return (group + step) % groups

    def behind(step):
        return (group + groups - step) % groups

    barrier = pltpu.get_barrier_semaphore()

    def greet(device):
        pl.semaphore_signal(
            barrier,
            inc=1,
            device_id=(device // subs, device % subs),
            device_id_type=pl.DeviceIdType.MESH,
        )

    greet(partner)

    @pl.loop(1, groups)
    def _(step):
        greet(member(ahead(step)))

    pl.semaphore_wait(barrier, groups)

    half_copy = remote(
        parts_ref.at[pl.ds(other * groups, groups)], half_in, half_sem.at[0], half_sem.at[1], partner
    )
    half_copy.start()
    node_copies = [
        remote(
            nodes_ref.at[2 * pair + other],
            node_in.at[pair],
            node_send.at[pair],
            node_recv.at[pair],
            partner,
        )
        for pair in range(sub_groups)
    ]
    for copy in node_copies:
        copy.start()
    half_copy.wait()

    def add_half(index):
        return parts_ref[parity * groups + index].astype(jnp.float32) + half_in[index].astype(
            jnp.float32
        )

    def group_copy(source, target):
        return remote(
            half_sum.at[target],
            group_in.at[source],
            group_send.at[target],
            group_recv.at[source],
            member(target),
        )

    @pl.loop(1, groups)
    def _(step):
        target = ahead(step)
        half_sum[target] = add_half(target).astype(half_sum.dtype)
        group_copy(group, target).start()

    for copy in node_copies:
        copy.wait()

    def last_copy(source, target):
        return remote(
            node_sum.at[target],
            node_last.at[source],
            last_send.at[target],
            last_recv.at[source],
            band * subs + 2 * target + parity,
        )

    def add_node(pair):
        return nodes_ref[2 * pair + parity].astype(jnp.float32) + node_in[pair].astype(jnp.float32)

    for step in range(1, sub_groups):
        target = (own_pair + step) % sub_groups
        node_sum[target] = add_node(target).astype(node_sum.dtype)
        last_copy(own_pair, target).start()

    def take(step, running):
        source = behind(step)
        group_copy(source, source).wait_recv()
        return running + group_in[source].astype(jnp.float32)

    mine = parity * groups + group
    total_ref[mine] = lax.fori_loop(1, groups, take, add_half(group)).astype(total_ref.dtype)

    def own_copy(source, target):
        place = total_ref.at[parity * groups + source]
        return remote(place, place, own_send.at[target], own_recv.at[source], member(target))

    def pass_copy(source, half):
        place = total_ref.at[half * groups + source]
        return remote(place, place, pass_send.at[source], pass_recv.at[source], partner)

    @pl.loop(1, groups)
    def _(step):
        own_copy(group, ahead(step)).start()

    pass_copy(group, parity).start()

    running = add_node(own_pair)
    for step in range(1, sub_groups):
        source = (own_pair + sub_groups - step) % sub_groups
        last_copy(source, source).wait_recv()
        running = running + node_last[source].astype(jnp.float32)
    node_ref[...] = running.astype(node_ref.dtype)

    @pl.loop(1, groups)
    def _(step):
        source = behind(step)
        own_copy(source, source).wait_recv()
        pass_copy(source, parity).start()

    @pl.loop(0, groups)
    def _(step):
        source = ahead(step)
        pass_copy(source, other).wait_recv()
        pass_copy(source, parity).wait_send()

    @pl.loop(1, groups)
    def _(step):
        target = ahead(step)
        group_copy(group, target).wait_send()
        own_copy(group, target).wait_send()

    for step in range(1, sub_groups):
        last_copy(own_pair, (own_pair + step) % sub_groups).wait_send()


def reduce_all(parts, nodes):
    devices, rows, columns = parts.shape
    subs, node_rows, width = nodes.shape
    groups, sub_groups = devices // 2, subs // 2
    vmem = pl.BlockSpec(memory_space=pltpu.VMEM)
    dma = pltpu.SemaphoreType.DMA
    return pl.pallas_call(
        functools.partial(reduce_kernel, subs),
        out_shape=(
            jax.ShapeDtypeStruct(parts.shape, parts.dtype),
            jax.ShapeDtypeStruct((node_rows, width), nodes.dtype),
        ),
        in_specs=[vmem, vmem],
        out_specs=(vmem, vmem),
        scratch_shapes=[pltpu.VMEM((groups, rows, columns), parts.dtype)] * 3
        + [pltpu.VMEM((sub_groups, node_rows, width), nodes.dtype)] * 3
        + [dma((2,))]
        + [dma((groups,))] * 6
        + [dma((sub_groups,))] * 4,
        compiler_params=pltpu.CompilerParams(collective_id=0, has_side_effects=True),
    )(parts, nodes)


def shards(grad_pred, grid_latent, mesh_latent, send_slot, edge_src, w_mesh, w_grid, w_msg, w_out):
    both = ("band", "sub")
    grid_rows, width = grid_latent.shape
    channels = grad_pred.shape[0]
    devices = lax.axis_size(both)
    subs = lax.axis_size("sub")
    capacity = 3 * grid_rows // devices
    total_points = grid_rows * devices
    slots = devices * capacity
    own_index = lax.axis_index(both)
    points = own_index * grid_rows + jnp.arange(grid_rows, dtype=jnp.int32)
    weighted = (
        latitude_weight(points, total_points)[None, :] * grad_pred.astype(jnp.float32)
    ).astype(jnp.bfloat16)
    padding = -channels % 128
    weighted = jnp.pad(weighted, ((0, padding), (0, 0)))
    w_out = jnp.pad(w_out, ((0, 0), (0, padding)))
    patch_latent = lax.all_gather(mesh_latent, "sub", axis=0, tiled=True)
    one_hot = spread(grid_latent, send_slot, slots)
    latent_send = jnp.dot(one_hot, grid_latent, preferred_element_type=jnp.float32).astype(
        jnp.bfloat16
    )
    grad_send = times_transpose(one_hot, weighted).astype(jnp.bfloat16)
    latent_rows = lax.all_to_all(
        latent_send.reshape(devices, capacity, width),
        both,
        split_axis=0,
        concat_axis=0,
        tiled=True,
    ).reshape(slots, width)
    grad_rows = lax.all_to_all(
        grad_send.reshape(devices, capacity, channels + padding),
        both,
        split_axis=0,
        concat_axis=0,
        tiled=True,
    ).reshape(slots, channels + padding)
    patch_size = patch_latent.shape[0]
    patch_proj = jnp.dot(patch_latent, w_mesh, preferred_element_type=jnp.float32).astype(
        jnp.bfloat16
    )
    local_node = edge_src - lax.axis_index("band") * patch_size
    nodes = lax.broadcasted_iota(jnp.int32, (slots, patch_size), 1)
    grid_float = (
        jnp.dot(latent_rows, w_grid, preferred_element_type=jnp.float32)
        .astype(jnp.bfloat16)
        .astype(jnp.float32)
    )
    pre_acts = [
        jnp.dot(
            (nodes == local_node[corner][:, None]).astype(jnp.bfloat16),
            patch_proj,
            preferred_element_type=jnp.float32,
        )
        + grid_float
        for corner in range(3)
    ]
    act_sum = (
        jax.nn.silu(pre_acts[0]) + jax.nn.silu(pre_acts[1]) + jax.nn.silu(pre_acts[2])
    ).astype(jnp.bfloat16)
    aggregate = jnp.dot(act_sum, w_msg, preferred_element_type=jnp.float32).astype(jnp.bfloat16)
    out_part = contract_rows(aggregate, grad_rows)
    agg_rows = times_transpose(grad_rows, w_out).astype(jnp.bfloat16)
    msg_part = contract_rows(act_sum, agg_rows)
    act_grad = times_transpose(agg_rows, w_msg)
    pre_grads = [(act_grad * silu_slope(pre)).astype(jnp.bfloat16) for pre in pre_acts]
    grid_proj_grad = (
        pre_grads[0].astype(jnp.float32)
        + pre_grads[1].astype(jnp.float32)
        + pre_grads[2].astype(jnp.float32)
    ).astype(jnp.bfloat16)
    targets = lax.broadcasted_iota(jnp.int32, (patch_size, slots), 0)
    node_part = sum(
        jnp.dot(
            (targets == local_node[corner][None, :]).astype(jnp.bfloat16),
            pre_grads[corner],
            preferred_element_type=jnp.float32,
        )
        for corner in range(3)
    ).astype(jnp.bfloat16)
    grid_part = contract_rows(latent_rows, grid_proj_grad)
    mesh_part = contract_rows(patch_latent, node_part)
    parts = jnp.concatenate([mesh_part, grid_part, msg_part, out_part], axis=1).astype(jnp.bfloat16)
    totals, mesh_proj_grad = reduce_all(
        parts.reshape(devices, width // devices, parts.shape[1]),
        node_part.reshape(subs, patch_size // subs, width),
    )
    totals = totals.reshape(parts.shape)
    mesh_grad = times_transpose(mesh_proj_grad, w_mesh).astype(jnp.bfloat16)
    grad_scale = 1.0 / math.sqrt(3.0 * total_points)
    scaled = totals.astype(jnp.float32) * grad_scale
    return (
        mesh_grad,
        scaled[:, :width],
        scaled[:, width : 2 * width],
        scaled[:, 2 * width : 3 * width],
        scaled[:, 3 * width : 3 * width + channels],
    )


def solution(mesh):
    placed = (
        P(None, ("band", "sub")),
        P(("band", "sub"), None),
        P(("band", "sub"), None),
        P(("band", "sub")),
        P(None, ("band", "sub")),
        P(),
        P(),
        P(),
        P(),
    )
    return jax.shard_map(
        shards,
        mesh=mesh,
        in_specs=placed,
        out_specs=(P(("band", "sub"), None), P(), P(), P(), P()),
        check_vma=False,
    )
```
